8 devices in a mesh: data: 1 (over z), ffn: 2 (over y), hid: 4 (over x, core).
Axes of the slice: x: 2, y: 2, z: 1, core: 2. Of those that a mesh axis runs over, the one named last changes fastest.
Arguments:
- residual: bfloat16 [64, 4096], P('data', 'hid')
- gain_mlp: float32 [4096], P('hid')
- gain_attn: float32 [4096], P('hid')
- w_gate: bfloat16 [4096, 11008], P('hid', 'ffn')
- w_up: bfloat16 [4096, 11008], P('hid', 'ffn')
- w_down: bfloat16 [11008, 4096], P('ffn', 'hid')
- w_qkv: bfloat16 [4096, 12288], P('hid', 'ffn')
Outputs:
- output 1: bfloat16 [64, 4096], P('data', 'hid')
- output 2: bfloat16 [64, 12288], P('data', 'ffn')
All inputs are finite; a program needn't handle non-finite values.
Results may differ from the reference program's by a relative error of at most 0.0185647.
Values are sent between devices in bfloat16 or wider.
A program may use at most 1 GiB of HBM per device.

```python
import jax
import jax.numpy as jnp
from jax import lax

TOKENS = 64
D_MODEL = 4096
D_FF = 11008
Q_HEADS = 32
KV_HEADS = 32
HEAD_DIM = 128
HID_WAYS = 4
FFN_WAYS = 2
QKV_DIM = (Q_HEADS + 2 * KV_HEADS) * HEAD_DIM
NORM_EPS = 1e-6


def setup_inputs(seed: int = 0, part: int = 0) -> dict:
    keys = jax.random.split(jax.random.key(seed), 8)
    part_keys = jax.random.split(jax.random.fold_in(keys[0], part), 4)
    d_shard = D_MODEL // HID_WAYS
    noise = jax.random.normal(part_keys[0], (TOKENS, HID_WAYS, d_shard), jnp.float32)
    row_scale = jnp.exp(jax.random.uniform(part_keys[1], (TOKENS, 1, 1), jnp.float32, minval=-1.0, maxval=1.0))
    block_scale = jnp.exp(jax.random.uniform(part_keys[2], (TOKENS, HID_WAYS, 1), jnp.float32, minval=-0.7, maxval=0.7))
    col_scale = jnp.exp(0.3 * jax.random.normal(part_keys[3], (HID_WAYS, d_shard), jnp.float32))
    residual = (noise * row_scale * block_scale * col_scale).reshape(TOKENS, D_MODEL)
    gain_mlp = jax.random.uniform(keys[1], (D_MODEL,), jnp.float32, minval=0.5, maxval=1.5)
    gain_attn = jax.random.uniform(keys[2], (D_MODEL,), jnp.float32, minval=0.5, maxval=1.5)
    w_gate = jax.random.normal(keys[3], (D_MODEL, D_FF), jnp.float32) * D_MODEL ** -0.5
    w_up = jax.random.normal(keys[4], (D_MODEL, D_FF), jnp.float32) * D_MODEL ** -0.5
    w_down = jax.random.normal(keys[5], (D_FF, D_MODEL), jnp.float32) * (2.0 * D_FF ** -0.5)
    w_qkv = jax.random.normal(keys[6], (D_MODEL, QKV_DIM), jnp.float32) * D_MODEL ** -0.5
    return dict(residual=residual.astype(jnp.bfloat16), gain_mlp=gain_mlp, gain_attn=gain_attn,
                w_gate=w_gate.astype(jnp.bfloat16), w_up=w_up.astype(jnp.bfloat16),
                w_down=w_down.astype(jnp.bfloat16), w_qkv=w_qkv.astype(jnp.bfloat16))


def rms_norm(resid_rows, gain):
    resid32 = resid_rows.astype(jnp.float32)
    sum_sq = jnp.sum(resid32 * resid32, axis=1, keepdims=True)
    scale = lax.rsqrt(sum_sq / resid_rows.shape[1] + NORM_EPS)
    return (resid32 * scale * gain[None, :]).astype(jnp.bfloat16)


def block_sum(left_mat, right_mat, ways):
    row_count = left_mat.shape[0]
    inner_dim = left_mat.shape[1] // ways
    left_blocks = jnp.transpose(left_mat.reshape(row_count, ways, inner_dim), (1, 0, 2))
    right_blocks = right_mat.reshape(ways, inner_dim, right_mat.shape[1])

    def add_piece(running, pair):
        piece = jnp.dot(pair[0], pair[1], preferred_element_type=jnp.float32).astype(jnp.bfloat16)
        return running + piece.astype(jnp.float32), None

    start_sum = jnp.zeros((row_count, right_mat.shape[1]), jnp.float32)
    summed, _ = lax.scan(add_piece, start_sum, (left_blocks, right_blocks))
    return summed.astype(jnp.bfloat16)


def reference(residual, gain_mlp, gain_attn, w_gate, w_up, w_down, w_qkv):
    normed = rms_norm(residual, gain_mlp)
    gate_sum = block_sum(normed, w_gate, HID_WAYS)
    up_sum = block_sum(normed, w_up, HID_WAYS)
    hidden_act = (jax.nn.silu(gate_sum.astype(jnp.float32)) * up_sum.astype(jnp.float32)).astype(jnp.bfloat16)
    down_sum = block_sum(hidden_act, w_down, FFN_WAYS)
    residual_out = (residual.astype(jnp.float32) + down_sum.astype(jnp.float32)).astype(jnp.bfloat16)
    normed_next = rms_norm(residual_out, gain_attn)
    qkv_out = block_sum(normed_next, w_qkv, HID_WAYS)
    return (residual_out, qkv_out)
```

```python
import jax
import jax.numpy as jnp
from jax import lax
from jax.experimental import pallas as pl
from jax.experimental.pallas import tpu as pltpu
from jax.sharding import PartitionSpec as P

NORM_EPS = 1e-6
F32 = jnp.float32
BF16 = jnp.bfloat16
MESH = pl.DeviceIdType.MESH

ROWS = 64
DW = 1024
FF = 5504
QW = 6144
D_MODEL = 4096
G = 2
T = ROWS // G
H = T // 2
Q = T // 4
W = 512
NC = 11
LAST = FF - W
WQ = 1024
NQ = QW // WQ
AHEAD = 4


def kernel(x_hbm, g1_hbm, g2_hbm, wg_hbm, wu_hbm, wd_hbm, wq_hbm,
           x2_out, q_out,
           wg, wu, wd, wq, xv, g1, g2, nv, x2v, n2v,
           part, recv1, xsend, recv2, abuf, acc, dsend, drecv,
           ss_send, ss_recv, qpart, qrecv1, qx, qrecv2,
           s_in, s_wg, s_wu, s_wd, s_wq,
           d1s, d1r, rss, rsr, ags, agr, fws, fwr, ys, yr, sss, ssr,
           qds, qdr, qxs, qxr, qfs, qfr, s_x2):
    f = lax.axis_index('ffn')
    h = lax.axis_index('hid')
    xi, c = h // 2, h % 2
    mate = xi * 2 + (1 - c)
    across = (1 - xi) * 2 + c
    cross = (1 - xi) * 2 + (1 - c)
    pos = 2 * c + xi

    def rdma(src, dst, ssem, rsem, **dev):
        return pltpu.make_async_remote_copy(
            src_ref=src, dst_ref=dst, send_sem=ssem, recv_sem=rsem,
            device_id=dev, device_id_type=MESH)

    ld_x = pltpu.make_async_copy(x_hbm, xv, s_in.at[0])
    ld_g1 = pltpu.make_async_copy(g1_hbm, g1, s_in.at[1])
    ld_g2 = pltpu.make_async_copy(g2_hbm, g2, s_in.at[2])

    def col(i):
        return pl.multiple_of(jnp.minimum(i * W, LAST), 128)

    def ld_wg(i):
        return pltpu.make_async_copy(wg_hbm.at[:, pl.ds(col(i), W)], wg.at[i], s_wg.at[i])

    def ld_wu(i):
        return pltpu.make_async_copy(wu_hbm.at[:, pl.ds(col(i), W)], wu.at[i], s_wu.at[i])

    def ld_wd(i):
        return pltpu.make_async_copy(wd_hbm.at[pl.ds(col(i), W), :], wd.at[i], s_wd.at[i])

    def ld_wq(k):
        return pltpu.make_async_copy(
            wq_hbm.at[:, pl.ds(pl.multiple_of(k * WQ, WQ), WQ)], wq.at[k], s_wq.at[k])

    ld_x.start()
    ld_g1.start()

    @pl.loop(0, AHEAD)
    def _(i):
        ld_wg(i).start()
        ld_wu(i).start()

    ld_g2.start()

    barrier = pltpu.get_barrier_semaphore()
    for dev in ({'hid': mate}, {'hid': across}, {'hid': cross}, {'ffn': 1 - f}):
        pl.semaphore_signal(barrier, inc=1, device_id=dev, device_id_type=MESH)

    def ss_copies(e):
        return [rdma(ss_send.at[e], ss_recv.at[e, j], sss.at[e, j], ssr.at[e, j], hid=dev)
                for j, dev in enumerate((mate, across, cross))]

    def ss_put(e, rows32):
        n_rows = rows32.shape[0]
        row = jnp.sum(rows32 * rows32, axis=1, keepdims=True)
        eye = (lax.broadcasted_iota(jnp.int32, (n_rows, 128), 0)
               == lax.broadcasted_iota(jnp.int32, (n_rows, 128), 1))
        ss_send[e] = jnp.sum(jnp.where(eye, row, 0.0), axis=0, keepdims=True)

    def ss_get(e, n_rows):
        for cp in ss_copies(e):
            cp.wait_recv()
        tot = (ss_send[e] + ss_recv[e, 0]) + (ss_recv[e, 1] + ss_recv[e, 2])
        eye = (lax.broadcasted_iota(jnp.int32, (n_rows, 128), 0)
               == lax.broadcasted_iota(jnp.int32, (n_rows, 128), 1))
        full = jnp.sum(jnp.where(eye, tot, 0.0), axis=1, keepdims=True)
        return lax.rsqrt(full / D_MODEL + NORM_EPS)

    ld_x.wait()
    ss_put(0, xv[...].astype(F32))
    pl.semaphore_wait(barrier, 4)
    for cp in ss_copies(0):
        cp.start()
    ld_g1.wait()
    ld_g2.wait()
    scale = ss_get(0, ROWS)
    nv[...] = (xv[...].astype(F32) * scale * g1[...]).astype(BF16)

    def d1(i):
        return rdma(part.at[i, 1 - c], recv1.at[i], d1s.at[i], d1r.at[i], hid=mate)

    def rs(g, i):
        return rdma(xsend.at[g, i, 1 - xi], recv2.at[g, i], rss.at[g, i], rsr.at[g, i], hid=across)

    def ag(g, i):
        return rdma(abuf.at[g, i, pos], abuf.at[g, i, pos], ags.at[g, i], agr.at[g, i], hid=across)

    def fw(g, i):
        return rdma(abuf.at[g, i, pl.ds(2 * c, 2)], abuf.at[g, i, pl.ds(2 * c, 2)],
                    fws.at[g, i], fwr.at[g, i], hid=mate)

    def stage_gemm(i):
        @pl.when(i + AHEAD < NC)
        def _():
            ld_wg(i + AHEAD).start()
            ld_wu(i + AHEAD).start()

        @pl.when(i + AHEAD >= NC)
        def _():
            for j in range(3):
                k = (i + AHEAD - NC) * 3 + j

                @pl.when(k < NC)
                def _(k=k):
                    ld_wd(k).start()

        ld_wg(i).wait()
        ld_wu(i).wait()
        for u, w_ref in enumerate((wg, wu)):
            p = jnp.dot(nv[...], w_ref[i], preferred_element_type=F32).astype(BF16)
            for g in range(G):
                for half in range(2):
                    r = g * T + half * H
                    part[i, half, g, u] = p[r:r + H]
        d1(i).start()

    def stage_core_sum(i):
        d1(i).wait_recv()
        for g in range(G):
            s = [part[i, c, g, u].astype(F32) + recv1[i, g, u].astype(F32) for u in range(2)]
            for v in range(2):
                xsend[g, i, v] = jnp.concatenate(
                    [s[0][v * Q:(v + 1) * Q], s[1][v * Q:(v + 1) * Q]], axis=0).astype(BF16)

    def stage_act(g, i):
        rs(g, i).wait_recv()
        tot = (xsend[g, i, xi].astype(F32) + recv2[g, i].astype(F32)).astype(BF16).astype(F32)
        a = jax.nn.silu(tot[:Q]) * tot[Q:]
        lane = lax.broadcasted_iota(jnp.int32, (Q, W), 1)
        dup = jnp.where(i == NC - 1, NC * W - FF, 0)
        abuf[g, i, pos] = jnp.where(lane < dup, 0.0, a).astype(BF16)
        ag(g, i).start()

    def stage_forward(g, i):
        ag(g, i).wait_recv()
        fw(g, i).start()

    def stage_down(g, i):
        @pl.when(g == 0)
        def _():
            ld_wd(i).wait()

        fw(g, i).wait_recv()
        a = abuf[g, i].astype(F32).reshape(T, W).astype(BF16)
        acc[g] += jnp.dot(a, wd[i], preferred_element_type=F32)

    def yx(g):
        return rdma(dsend.at[g], drecv.at[g], ys.at[g], yr.at[g], ffn=1 - f)

    def down_send(g):
        dsend[g] = acc[g].astype(BF16)
        yx(g).start()

    def resid(g):
        yx(g).wait_recv()
        dn = (dsend[g].astype(F32) + drecv[g].astype(F32)).astype(BF16).astype(F32)
        x2 = (xv[g * T:(g + 1) * T].astype(F32) + dn).astype(BF16)
        x2v[g * T:(g + 1) * T] = x2
        ss_put(1 + g, x2.astype(F32))
        for cp in ss_copies(1 + g):
            cp.start()

    def norm2(g):
        s2 = ss_get(1 + g, T)
        n2v[g] = (x2v[g * T:(g + 1) * T].astype(F32) * s2 * g2[...]).astype(BF16)

    acc[...] = jnp.zeros_like(acc)

    LA, LB = 5, NC + 1
    SA = (LA, LA + 3, LA + 5)
    SB = (LB + 5, LB + 8, LB + 10)
    RES0 = SA[2] + NC + 6
    NRM0 = RES0 + 4
    END = SB[2] + NC

    def at(i, lag, fn):
        k = i - lag

        @pl.when(jnp.logical_and(k >= 0, k < NC))
        def _():
            fn(k)

    @pl.loop(0, END)
    def _(i):
        at(i, 0, stage_gemm)

        def sum_send(k):
            stage_core_sum(k)
            rs(0, k).start()
        at(i, 1, sum_send)
        at(i, LB, lambda k: rs(1, k).start())
        at(i, LB, lambda k: pl.when(k < NQ)(lambda: ld_wq(k).start()))
        at(i, SA[0], lambda k: stage_act(0, k))
        at(i, SA[1], lambda k: stage_forward(0, k))
        at(i, SA[2], lambda k: stage_down(0, k))
        pl.when(i == SA[2] + NC - 1)(lambda: down_send(0))
        at(i, SB[0], lambda k: stage_act(1, k))
        at(i, SB[1], lambda k: stage_forward(1, k))
        at(i, SB[2], lambda k: stage_down(1, k))
        pl.when(i == RES0)(lambda: resid(0))
        pl.when(i == NRM0)(lambda: norm2(0))

    down_send(1)

    def qd(g, k):
        return rdma(qpart.at[g, k, 1 - c], qrecv1.at[g, k], qds.at[g, k], qdr.at[g, k], hid=mate)

    def qe(g, k):
        return rdma(qx.at[g, k], qrecv2.at[g, k], qxs.at[g, k], qxr.at[g, k], hid=across)

    def qcols(k):
        return pl.ds(pl.multiple_of(k * WQ, WQ), WQ)

    def qf(g, k):
        ref = q_out.at[pl.ds(pl.multiple_of(g * T + c * H, H), H), qcols(k)]
        return rdma(ref, ref, qfs.at[g, k], qfr.at[g, k], hid=mate)

    def q_gemm(g, k):
        if g == 0:
            ld_wq(k).wait()
        p = jnp.dot(n2v[g], wq[k], preferred_element_type=F32).astype(BF16)
        for half in range(2):
            qpart[g, k, half] = p[half * H:(half + 1) * H]
        qd(g, k).start()

    def q_sum(g, k):
        qd(g, k).wait_recv()
        qx[g, k] = (qpart[g, k, c].astype(F32) + qrecv1[g, k].astype(F32)).astype(BF16)
        qe(g, k).start()

    def q_fin(g, k):
        qe(g, k).wait_recv()
        v = (qx[g, k].astype(F32) + qrecv2[g, k].astype(F32)).astype(BF16)
        q_out[pl.ds(pl.multiple_of(g * T + c * H, H), H), qcols(k)] = v
        qf(g, k).start()

    def q_push(g):
        @pl.loop(0, NQ + 1)
        def _(k):
            pl.when(k < NQ)(lambda: q_gemm(g, k))
            pl.when(k > 0)(lambda: q_sum(g, k - 1))

    q_push(0)
    resid(1)
    x2_out[...] = x2v[...]
    pl.loop(0, 2)(lambda k: q_fin(0, k))
    norm2(1)
    q_push(1)
    pl.loop(2, NQ)(lambda k: q_fin(0, k))
    pl.loop(0, NQ)(lambda k: q_fin(1, k))

    @pl.loop(0, NQ)
    def _(k):
        for g in range(G):
            qf(g, k).wait_recv()
            qf(g, k).wait_send()
            qd(g, k).wait_send()
            qe(g, k).wait_send()

    @pl.loop(0, NC)
    def _(i):
        d1(i).wait_send()
        for g in range(G):
            rs(g, i).wait_send()
            ag(g, i).wait_send()
            fw(g, i).wait_send()

    for g in range(G):
        yx(g).wait_send()
    for e in range(1 + G):
        for cp in ss_copies(e):
            cp.wait_send()


def solution(mesh):
    def device_step(residual, gain_mlp, gain_attn, w_gate, w_up, w_down, w_qkv):
        V = pltpu.VMEM
        D = pltpu.SemaphoreType.DMA
        scratch = [
            V((NC, DW, W), BF16), V((NC, DW, W), BF16), V((NC, W, DW), BF16), V((NQ, DW, WQ), BF16),
            V((ROWS, DW), BF16), V((1, DW), F32), V((1, DW), F32),
            V((ROWS, DW), BF16), V((ROWS, DW), BF16), V((G, T, DW), BF16),
            V((NC, 2, G, 2, H, W), BF16), V((NC, G, 2, H, W), BF16),
            V((G, NC, 2, 2 * Q, W), BF16), V((G, NC, 2 * Q, W), BF16),
            V((G, NC, 4, Q, W), BF16), V((G, T, DW), F32), V((G, T, DW), BF16), V((G, T, DW), BF16),
            V((1 + G, 1, 128), F32), V((1 + G, 3, 1, 128), F32),
            V((G, NQ, 2, H, WQ), BF16), V((G, NQ, H, WQ), BF16), V((G, NQ, H, WQ), BF16),
            V((G, NQ, H, WQ), BF16),
            D((3,)), D((NC,)), D((NC,)), D((NC,)), D((NQ,)),
            D((NC,)), D((NC,)),
            D((G, NC)), D((G, NC)), D((G, NC)), D((G, NC)), D((G, NC)), D((G, NC)),
            D((G,)), D((G,)), D((1 + G, 3)), D((1 + G, 3)),
            D((G, NQ)), D((G, NQ)), D((G, NQ)), D((G, NQ)), D((G, NQ)), D((G, NQ)), D((1,)),
        ]
        any_spec = pl.BlockSpec(memory_space=pl.ANY)
        vmem_spec = pl.BlockSpec(memory_space=pltpu.VMEM)
        return pl.pallas_call(
            kernel,
            out_shape=(jax.ShapeDtypeStruct((ROWS, DW), BF16), jax.ShapeDtypeStruct((ROWS, QW), BF16)),
            in_specs=[any_spec] * 7,
            out_specs=(vmem_spec, vmem_spec),
            scratch_shapes=scratch,
            compiler_params=pltpu.CompilerParams(
                collective_id=0, has_side_effects=True, vmem_limit_bytes=67_000_000),
        )(residual, gain_mlp[None, :], gain_attn[None, :], w_gate, w_up, w_down, w_qkv)

    return jax.shard_map(
        device_step, mesh=mesh,
        in_specs=(P('data', 'hid'), P('hid'), P('hid'), P('hid', 'ffn'), P('hid', 'ffn'),
                  P('ffn', 'hid'), P('hid', 'ffn')),
        out_specs=(P('data', 'hid'), P('data', 'ffn')),
        check_vma=False)
```
